32 devices in a mesh: rep: 2 (over y), seq: 4 (over z), head: 4 (over x, core).
Axes of the slice: x: 2, y: 2, z: 4, core: 2. Of those that a mesh axis runs over, the one named last changes fastest.
Arguments:
- queries: bfloat16 [2048, 4096], P(('rep', 'seq'), 'head'), parts along dimension 0, may hold values from -520 to 520
- rotated_key_states: bfloat16 [2048, 1024], P(('rep', 'seq'), 'head'), parts along dimension 0, may hold values from -6 to 6
- value_state_array: bfloat16 [2048, 1024], P(('rep', 'seq'), 'head'), parts along dimension 0, may hold values from -6 to 6
- residual: bfloat16 [2048, 4096], P(('rep', 'seq'), 'head'), parts along dimension 0, may hold values from -60 to 60
- out_weight: bfloat16 [4096, 4096], P('head'), may hold values from -0.75 to 0.75
- norm_gain: bfloat16 [4096], P('head'), may hold values from 0.5 to 1.5
- block_order: int32 [16], P('rep'), parts along dimension 0, may hold values from 0 to 7, as said below
Outputs:
- normed: bfloat16 [2048, 4096], P(('rep', 'seq'), 'head'), parts along dimension 0
The draws below stay inside these ranges and needn't reach their ends.
There are 2 independent parts, one for each index of `rep`. The reference program is written for one: setup_inputs(seed, part) draws one part's arguments, and reference() takes and returns one part's arrays. A program takes and returns all parts, laid end to end along the dimension named above; an argument that names none is the same for every part. Nothing has to cross between parts.
Inputs may be any that keep to these rules, and one draw needn't show every extreme that they name: `block_order`: slots 2i and 2i + 1 hold blocks c and 7 - c in either order; every block appears once.
All inputs are finite; a program needn't handle non-finite values.
Results may differ from the reference program's by a relative error of at most 0.008.
Values may be sent and summed in bfloat16 or wider, within the bound.
No kernel may reach another device: no remote copies, remote signals or barrier semaphores. Data moves between devices by JAX's collectives and lax.ppermute only.
A program may use at most 64 MiB of HBM per device.

```python
import math
import jax
import jax.numpy as jnp
from jax import lax

D = 4096
QUERY_HEADS = 32
KEY_VALUE_HEADS = 8
HEAD_SIZE = 128
SEQUENCE_BLOCK = 128
BLOCKS = 8
SEQUENCE_LENGTH = 1024


def paired_heads(key):
    base_key = jax.random.fold_in(key, 7)
    query_key, random_key_for_keys = jax.random.split(base_key, 2)
    unrotated_queries = jnp.clip(jax.random.normal(query_key, (SEQUENCE_LENGTH, QUERY_HEADS * HEAD_SIZE), jnp.float32) * 1.5, -9.0, 9.0)
    unrotated_keys = jnp.clip(jax.random.normal(random_key_for_keys, (SEQUENCE_LENGTH, KEY_VALUE_HEADS, HEAD_SIZE), jnp.float32), -6.0, 6.0)
    return (unrotated_queries, unrotated_keys.reshape(SEQUENCE_LENGTH, KEY_VALUE_HEADS * HEAD_SIZE))


def draw_queries(key, part):
    return paired_heads(key)[0].astype(jnp.bfloat16)


def draw_rotated_key_states(key, part):
    return paired_heads(key)[1].astype(jnp.bfloat16)


def draw_residual(key, part):
    row_key, column_key, entry_key = jax.random.split(jax.random.fold_in(key, 5), 3)
    row_scale = jnp.exp(jax.random.uniform(row_key, (SEQUENCE_LENGTH, 1), jnp.float32, math.log(0.3), math.log(3.0)))
    column_place = jnp.arange(D, dtype=jnp.float32) / D
    jitter = jax.random.uniform(column_key, (D,), jnp.float32, 0.7, 1.3)
    column_scale = jnp.power(3.0, column_place) * jitter
    entries = jnp.clip(jax.random.normal(entry_key, (SEQUENCE_LENGTH, D), jnp.float32), -5.0, 5.0)
    return (entries * row_scale * column_scale[None, :]).astype(jnp.bfloat16)


def draw_block_order(key, part):
    pair_key, flip_key = jax.random.split(jax.random.fold_in(key, 3))
    pair_count = BLOCKS // 2
    early_ids = jax.random.permutation(pair_key, pair_count).astype(jnp.int32)
    flip_bits = jax.random.randint(flip_key, (pair_count,), 0, 2)
    first_slot = jnp.where(flip_bits == 1, early_ids, BLOCKS - 1 - early_ids)
    second_slot = BLOCKS - 1 - first_slot
    return jnp.stack([first_slot, second_slot], axis=1).reshape(BLOCKS).astype(jnp.int32)


def level_of(own_key, shape, cuts, least, largest):
    factor_of, own = 1.0, jax.random.fold_in(own_key, 6)
    for dim, blocks in cuts:
        heights = jnp.exp(jax.random.uniform(jax.random.fold_in(own, dim), (blocks,), jnp.float32, least / len(cuts), largest / len(cuts)))
        factor_of = factor_of * jnp.repeat(heights, shape[dim] // blocks).reshape([-1 if axis == dim else 1 for axis in range(len(shape))])
    return factor_of


def centred(key, dims, deviation, reach, shards=(), kind=jnp.bfloat16):
    drawn = deviation * jax.random.normal(key, dims, jnp.float32)
    if shards:
        drawn = drawn * level_of(key, dims, shards, -0.22, 0.18)
    return jnp.clip(drawn, -reach, reach).astype(kind)


def setup_inputs(seed: int = 0, part: int = 0) -> dict:
    key_list = jax.random.split(jax.random.key(seed), 8)
    part_splits = jax.random.split(jax.random.fold_in(key_list[7], part), 8)
    return {
        "queries": draw_queries(jax.random.fold_in(jax.random.fold_in(key_list[7], part), 71), part),
        "rotated_key_states": draw_rotated_key_states(jax.random.fold_in(jax.random.fold_in(key_list[7], part), 71), part),
        "value_state_array": centred(part_splits[2], (SEQUENCE_LENGTH, KEY_VALUE_HEADS * HEAD_SIZE), 1.0, 6.0, ((0, 4), (1, 4))),
        "residual": draw_residual(jax.random.fold_in(jax.random.fold_in(key_list[7], part), 71), part),
        "out_weight": centred(key_list[4], (QUERY_HEADS * HEAD_SIZE, D), (HEAD_SIZE // 2) ** -0.5, 0.75, ((0, 4),)),
        "norm_gain": jnp.clip(1.0 + 0.1 * jax.random.normal(key_list[5], (D,), jnp.float32), 0.5, 1.5).astype(jnp.bfloat16),
        "block_order": draw_block_order(jax.random.fold_in(jax.random.fold_in(key_list[7], part), 71), part),
    }


norm_epsilon = 1e-05

def reference(queries, rotated_key_states, value_state_array, residual, out_weight, norm_gain, block_order):
    row_total_count = queries.shape[0]
    row_ids = jnp.arange(row_total_count, dtype=jnp.int32)
    positions = (block_order[row_ids // SEQUENCE_BLOCK] * SEQUENCE_BLOCK + row_ids % SEQUENCE_BLOCK).astype(jnp.int32)
    queries_per_group = QUERY_HEADS // KEY_VALUE_HEADS
    heads_of_keys = rotated_key_states.astype(jnp.float32).reshape(row_total_count, KEY_VALUE_HEADS, HEAD_SIZE)
    heads_of_values = value_state_array.astype(jnp.float32).reshape(row_total_count, KEY_VALUE_HEADS, HEAD_SIZE)
    heads_of_queries = queries.astype(jnp.float32).reshape(row_total_count // SEQUENCE_BLOCK, SEQUENCE_BLOCK, KEY_VALUE_HEADS, queries_per_group, HEAD_SIZE)
    query_positions = positions.reshape(row_total_count // SEQUENCE_BLOCK, SEQUENCE_BLOCK)

    def one_block(packed):
        block_queries, block_positions = packed
        scores = jnp.einsum('qhgd,khd->hgqk', block_queries, heads_of_keys, precision=lax.Precision.HIGHEST) * HEAD_SIZE ** (-0.5)
        visible = (positions[None, :] <= block_positions[:, None])[None, None]
        limited = jnp.where(visible, scores, -1e+30)
        row_peak = lax.optimization_barrier(jnp.max(limited, axis=3, keepdims=True))
        weights = jnp.where(visible, jnp.exp(limited - row_peak), 0.0)
        denominators = lax.optimization_barrier(jnp.sum(weights, axis=3))
        rounded = lax.optimization_barrier(weights.astype(jnp.bfloat16)).astype(jnp.float32)
        weighted_sum = jnp.einsum('hgqk,khd->hgqd', rounded, heads_of_values, precision=lax.Precision.HIGHEST)
        result = weighted_sum / denominators[..., None]
        return result.transpose(2, 0, 1, 3).reshape(SEQUENCE_BLOCK, QUERY_HEADS * HEAD_SIZE).astype(jnp.bfloat16)
    attention = lax.map(one_block, (heads_of_queries, query_positions)).reshape(row_total_count, QUERY_HEADS * HEAD_SIZE)
    mixed_rows = residual.astype(jnp.float32) + jnp.dot(attention, out_weight, preferred_element_type=jnp.float32)
    mean_square = lax.optimization_barrier(jnp.mean(mixed_rows * mixed_rows, axis=1))
    inverse = lax.rsqrt(mean_square + norm_epsilon)
    return (mixed_rows * inverse[:, None] * norm_gain.astype(jnp.float32)[None, :]).astype(jnp.bfloat16)
```

```python
import functools
import math

import jax
import jax.numpy as jnp
from jax import lax
from jax.experimental import pallas as pl
from jax.experimental.pallas import tpu as pltpu
from jax.sharding import PartitionSpec as P

HEAD_SIZE = 128
norm_epsilon = 1e-05
FAR = -1e30
VMEM = pltpu.VMEM
SMEM = pltpu.SMEM
LIMIT = 40 * 2**20


def vmem_out(shape, dtype):
    return pltpu.VMEM(shape, dtype)


def whole(space):
    return pl.BlockSpec(memory_space=space)


def params():
    return pltpu.CompilerParams(vmem_limit_bytes=LIMIT)


def cost(flops, size, exps=0):
    return pl.CostEstimate(flops=flops, bytes_accessed=size, transcendentals=exps)


def early_of(order_ref, slot):
    return jnp.minimum(order_ref[2 * slot], order_ref[2 * slot + 1])


def flip_of(order_ref):
    me = lax.axis_index("seq")
    return (order_ref[2 * me] > order_ref[2 * me + 1]).astype(jnp.int32)


def half(index, rows):
    return pl.ds(pl.multiple_of(index * rows, rows), rows)


def split_kernel(order_ref, k_ref, v_ref, early_ref, late_ref):
    rows = early_ref.shape[0]
    width = k_ref.shape[1]
    flip = flip_of(order_ref)
    for out, index in ((early_ref, flip), (late_ref, 1 - flip)):
        out[:, :width] = k_ref[half(index, rows), :]
        out[:, width:] = v_ref[half(index, rows), :]


def split_halves(order, keys, values):
    rows, width = keys.shape[0] // 2, keys.shape[1]
    out = jax.ShapeDtypeStruct((rows, 2 * width), keys.dtype)
    return pl.pallas_call(
        split_kernel,
        out_shape=(out, out),
        in_specs=[whole(SMEM), whole(VMEM), whole(VMEM)],
        out_specs=(whole(VMEM), whole(VMEM)),
        compiler_params=params(),
        name="split_halves",
        cost_estimate=cost(1000, 1 << 20),
    )(order, keys, values)


def attend(q_rows, pieces, biases, diagonal, kv_heads):
    rows = q_rows.shape[0]
    width = kv_heads * HEAD_SIZE
    group = q_rows.shape[1] // width
    factor = HEAD_SIZE ** (-0.5) * math.log2(math.e)
    outs = []
    for h in range(kv_heads):
        lanes = slice(h * HEAD_SIZE, (h + 1) * HEAD_SIZE)
        v_lanes = slice(width + h * HEAD_SIZE, width + (h + 1) * HEAD_SIZE)
        keys = jnp.concatenate([p[:, lanes] for p in pieces], axis=0)
        vals = jnp.concatenate([p[:, v_lanes] for p in pieces], axis=0)
        heads = [
            q_rows[:, (h * group + g) * HEAD_SIZE : (h * group + g + 1) * HEAD_SIZE]
            for g in range(group)
        ]
        stacked = jnp.concatenate(heads, axis=0)
        scores = lax.dot_general(
            stacked, keys, (((1,), (1,)), ((), ())), preferred_element_type=jnp.float32
        )
        parts = []
        for j, bias in enumerate(biases):
            part = scores[:, j * rows : (j + 1) * rows]
            if bias is not None:
                part = part + bias
            parts.append(part)
        last = scores[:, len(biases) * rows :].reshape(group, rows, rows)
        parts.append(jnp.where(diagonal[None], last, FAR).reshape(group * rows, rows))
        peak = functools.reduce(jnp.maximum, parts)
        peak = jnp.max(peak, axis=1, keepdims=True)
        weights = [jnp.exp2((part - peak) * factor) for part in parts]
        total = jnp.sum(functools.reduce(jnp.add, weights), axis=1, keepdims=True)
        rounded = jnp.concatenate([w.astype(jnp.bfloat16) for w in weights], axis=1)
        mixed = lax.dot_general(
            rounded, vals, (((1,), (0,)), ((), ())), preferred_element_type=jnp.float32
        )
        mixed = (mixed / total).astype(jnp.bfloat16)
        outs += [mixed[g * rows : (g + 1) * rows] for g in range(group)]
    return jnp.concatenate(outs, axis=1)


def project(att, w_ref, away_ref, keep_ref, n_core):
    head = lax.axis_index("head")
    chip, core = head // n_core, head % n_core
    cols = away_ref.shape[1] // 2
    for i, owner_chip in enumerate((1 - chip, chip)):
        for ref, owner_core in ((away_ref, 1 - core), (keep_ref, core)):
            start = pl.multiple_of((owner_chip * n_core + owner_core) * cols, cols)
            block = jnp.dot(att, w_ref[:, pl.ds(start, cols)], preferred_element_type=jnp.float32)
            ref[:, i * cols : (i + 1) * cols] = block.astype(ref.dtype)


def side_kernel(late, kv_heads, n_core, order_ref, q_ref, w_ref, *refs):
    *piece_refs, away_ref, keep_ref = refs
    rows = away_ref.shape[0]
    me = lax.axis_index("seq")
    mine = early_of(order_ref, me)
    flip = flip_of(order_ref)
    q_rows = q_ref[half((1 - flip) if late else flip, rows), :]
    peers = [early_of(order_ref, me ^ p) for p in (1, 2, 3)]
    if late:
        biases = [None] * 4 + [jnp.where(c > mine, 0.0, FAR) for c in peers]
    else:
        biases = [jnp.where(c < mine, 0.0, FAR) for c in peers]
    row = lax.broadcasted_iota(jnp.int32, (rows, rows), 0)
    col = lax.broadcasted_iota(jnp.int32, (rows, rows), 1)
    att = attend(q_rows, [r[...] for r in piece_refs], biases, col <= row, kv_heads)
    project(att, w_ref, away_ref, keep_ref, n_core)


def side(late, kv_heads, n_core, order, queries, weight, pieces):
    rows, depth = queries.shape[0] // 2, queries.shape[1]
    cols = weight.shape[1] // 2
    keys = rows * len(pieces)
    flops = 4 * rows * depth * keys + 2 * rows * depth * weight.shape[1]
    return pl.pallas_call(
        functools.partial(side_kernel, late, kv_heads, n_core),
        out_shape=(
            jax.ShapeDtypeStruct((rows, cols), jnp.bfloat16),
            jax.ShapeDtypeStruct((rows, cols), jnp.float32),
        ),
        in_specs=[whole(SMEM)] + [whole(VMEM)] * (2 + len(pieces)),
        out_specs=(whole(VMEM), whole(VMEM)),
        compiler_params=params(),
        name="late_side" if late else "early_side",
        cost_estimate=cost(flops, 16 << 20, rows * depth * keys // HEAD_SIZE),
    )(order, queries, weight, *pieces)


def load_kernel(w_ref, out_ref, sem):
    copy = pltpu.make_async_copy(w_ref, out_ref, sem)
    copy.start()
    copy.wait()


def load_weights(weight):
    return pl.pallas_call(
        load_kernel,
        out_shape=vmem_out(weight.shape, weight.dtype),
        in_specs=[whole(pl.ANY)],
        out_specs=whole(VMEM),
        scratch_shapes=[pltpu.SemaphoreType.DMA],
        compiler_params=pltpu.CompilerParams(vmem_limit_bytes=12 * 2**20),
        name="load_weights",
        cost_estimate=cost(1 << 20, 16 << 20),
    )(weight)


def mix_kernel(late, order_ref, res_ref, keep_ref, core_ref, chip_ref, mixed_ref, sq_ref):
    rows = mixed_ref.shape[0]
    cols = mixed_ref.shape[1]
    flip = flip_of(order_ref)
    res = res_ref[half((1 - flip) if late else flip, rows), :].astype(jnp.float32)
    own = keep_ref[:, cols:] + core_ref[:, cols:].astype(jnp.float32)
    mixed = res + (own + chip_ref[...].astype(jnp.float32))
    mixed_ref[...] = mixed
    squares = mixed * mixed
    lanes = functools.reduce(
        jnp.add, [squares[:, j : j + rows] for j in range(0, cols, rows)]
    )
    sq_ref[...] = jnp.broadcast_to(jnp.sum(lanes.T, axis=0, keepdims=True), sq_ref.shape)


def mix(late, order, residual, keep, core, chip):
    rows, cols = residual.shape[0] // 2, residual.shape[1]
    return pl.pallas_call(
        functools.partial(mix_kernel, late),
        out_shape=(
            jax.ShapeDtypeStruct((rows, cols), jnp.float32),
            jax.ShapeDtypeStruct((8, rows), jnp.float32),
        ),
        in_specs=[whole(SMEM)] + [whole(VMEM)] * 4,
        out_specs=(whole(VMEM), whole(VMEM)),
        compiler_params=params(),
        name="late_mix" if late else "early_mix",
        cost_estimate=cost(1 << 20, 2 << 20),
    )(order, residual, keep, core, chip)


def final_kernel(features, order_ref, gain_ref, early_ref, late_ref, *refs):
    *sq_refs, out_ref = refs
    rows, cols = early_ref.shape
    flip = flip_of(order_ref)
    gain = gain_ref[...].astype(jnp.float32)
    totals = functools.reduce(jnp.add, [r[...] for r in sq_refs])
    for i, (ref, index) in enumerate(((early_ref, flip), (late_ref, 1 - flip))):
        inverse = lax.rsqrt(totals[8 * i : 8 * i + 1] / features + norm_epsilon)
        inverse = jnp.broadcast_to(inverse, (rows, rows)).T
        for j in range(0, cols, rows):
            block = ref[:, j : j + rows] * inverse * gain[:, j : j + rows]
            out_ref[half(index, rows), j : j + rows] = block.astype(out_ref.dtype)


def final(features, order, gain, early, late, sums):
    rows, cols = early.shape
    return pl.pallas_call(
        functools.partial(final_kernel, features),
        out_shape=jax.ShapeDtypeStruct((2 * rows, cols), jnp.bfloat16),
        in_specs=[whole(SMEM)] + [whole(VMEM)] * (3 + len(sums)),
        out_specs=whole(VMEM),
        compiler_params=params(),
        name="final_norm",
        cost_estimate=cost(1 << 20, 2 << 20),
    )(order, gain.reshape(1, cols), early, late, *sums)


def exchange(x, axis, size, step):
    return lax.ppermute(x, axis, [(i, i ^ step) for i in range(size)])


def paired_body(n_seq, n_head, n_core, queries, keys, values, residual, weight, gain, order):
    kv_heads = keys.shape[1] // HEAD_SIZE
    cols = residual.shape[1]
    early, late = split_halves(order, keys, values)
    seq = lambda x, step: exchange(x, "seq", n_seq, step)
    head = lambda x, step: exchange(x, "head", n_head, step)

    early_b = seq(early, 2)
    early_a = seq(early, 1)
    late_b = seq(late, 2)
    early_c = seq(early_b, 1)
    late_a = seq(late, 1)
    late_c = seq(late_b, 1)
    held = load_weights(weight)

    away_e, keep_e = side(
        False, kv_heads, n_core, order, queries, held, [early_a, early_b, early_c, early]
    )
    core_e = head(away_e, 1)
    chip_e = head((keep_e[:, :cols] + core_e[:, :cols].astype(jnp.float32)).astype(jnp.bfloat16), n_core)

    away_l, keep_l = side(
        True,
        kv_heads,
        n_core,
        order,
        queries,
        held,
        [early, early_a, early_b, early_c, late_a, late_b, late_c, late],
    )
    core_l = head(away_l, 1)
    chip_l = head((keep_l[:, :cols] + core_l[:, :cols].astype(jnp.float32)).astype(jnp.bfloat16), n_core)

    mixed_e, sq_e = mix(False, order, residual, keep_e, core_e, chip_e)
    mixed_l, sq_l = mix(True, order, residual, keep_l, core_l, chip_l)
    own = jnp.concatenate([sq_e, sq_l], axis=0)
    others = [head(own, step) for step in range(1, n_head)]
    return final(n_head * cols, order, gain, mixed_e, mixed_l, [own] + others)


def slot_positions(row_ids, block_order, block_rows):
    slot_index = row_ids // block_rows
    slot_ids = jnp.arange(block_order.shape[0], dtype=jnp.int32)
    starts = jnp.sum(
        jnp.where(slot_index[:, None] == slot_ids[None, :], block_order[None, :], 0), axis=1
    )
    return starts * block_rows + row_ids % block_rows


def attend_block(carried, query_rows, query_positions, key_block, value_block, key_positions):
    row_peak, denominators, weighted_sum = carried
    scores = jnp.einsum(
        "qhgd,khd->hgqk", query_rows, key_block, preferred_element_type=jnp.float32
    ) * HEAD_SIZE ** (-0.5)
    visible = (key_positions[None, :] <= query_positions[:, None])[None, None]
    scores = jnp.where(visible, scores, FAR)
    new_peak = jnp.maximum(row_peak, jnp.max(scores, axis=3))
    weights = jnp.where(visible, jnp.exp(scores - new_peak[..., None]), 0.0)
    factor = jnp.exp(row_peak - new_peak)
    denominators = denominators * factor + jnp.sum(weights, axis=3)
    weighted_sum = weighted_sum * factor[..., None] + jnp.einsum(
        "hgqk,khd->hgqd",
        weights.astype(jnp.bfloat16),
        value_block,
        preferred_element_type=jnp.float32,
    )
    return (new_peak, denominators, weighted_sum)


def gathered_body(n_head, queries, keys, values, residual, weight, gain, order):
    tok_rows = queries.shape[0]
    block_rows = tok_rows // 2
    kv_heads = keys.shape[1] // HEAD_SIZE
    q_heads = queries.shape[1] // HEAD_SIZE
    group = q_heads // kv_heads
    own_rows = lax.axis_index("seq") * tok_rows + jnp.arange(tok_rows, dtype=jnp.int32)
    own_positions = slot_positions(own_rows, order, block_rows)
    shaped = queries.reshape(tok_rows, kv_heads, group, HEAD_SIZE)
    all_keys = lax.all_gather(keys, "seq", axis=0, tiled=True)
    all_values = lax.all_gather(values, "seq", axis=0, tiled=True)
    count = all_keys.shape[0]
    width = math.gcd(count, 512)
    all_keys = all_keys.reshape(count, kv_heads, HEAD_SIZE)
    all_values = all_values.reshape(count, kv_heads, HEAD_SIZE)

    def one_step(index, state):
        offset = index * width
        row_ids = offset + jnp.arange(width, dtype=jnp.int32)
        return attend_block(
            state,
            shaped,
            own_positions,
            lax.dynamic_slice_in_dim(all_keys, offset, width, 0),
            lax.dynamic_slice_in_dim(all_values, offset, width, 0),
            slot_positions(row_ids, order, block_rows),
        )

    state = (
        jnp.full((kv_heads, group, tok_rows), FAR, jnp.float32),
        jnp.zeros((kv_heads, group, tok_rows), jnp.float32),
        jnp.zeros((kv_heads, group, tok_rows, HEAD_SIZE), jnp.float32),
    )
    _, denominators, weighted_sum = lax.fori_loop(0, count // width, one_step, state)
    att = (weighted_sum / denominators[..., None]).transpose(2, 0, 1, 3)
    att = att.reshape(tok_rows, q_heads * HEAD_SIZE).astype(jnp.bfloat16)
    partial_terms = jnp.dot(att, weight, preferred_element_type=jnp.float32)
    projected = lax.psum_scatter(
        partial_terms.astype(jnp.bfloat16), "head", scatter_dimension=1, tiled=True
    ).astype(jnp.float32)
    mixed = residual.astype(jnp.float32) + projected
    totals = lax.psum(jnp.sum(mixed * mixed, axis=1), "head")
    inverse = lax.rsqrt(totals / (n_head * residual.shape[1]) + norm_epsilon)
    return (mixed * inverse[:, None] * gain.astype(jnp.float32)[None, :]).astype(jnp.bfloat16)


def solution(mesh):
    n_seq, n_head = mesh.shape["seq"], mesh.shape["head"]
    rows, wide = P(("rep", "seq"), "head"), P("head", None)
    in_specs = (rows, rows, rows, rows, wide, P("head"), P("rep"))
    if n_seq == 4 and n_head == 4:
        body = functools.partial(paired_body, n_seq, n_head, n_head // 2)
    else:
        body = functools.partial(gathered_body, n_head)
    return jax.shard_map(body, mesh=mesh, in_specs=in_specs, out_specs=rows, check_vma=False)
```

```python
import functools
import math

import jax
import jax.numpy as jnp
from jax import lax
from jax.experimental import pallas as pl
from jax.experimental.pallas import tpu as pltpu
from jax.sharding import PartitionSpec as P


HEAD_SIZE = 128
norm_epsilon = 1e-05
FAR = -1e30
VMEM = pltpu.VMEM
SMEM = pltpu.SMEM
HBM = pltpu.HBM
LIMIT = 40 * 2**20


def vmem_out(shape, dtype):
    return pltpu.VMEM(shape, dtype)


def in_hbm(*arrays):
    return [pltpu.with_memory_space_constraint(x, HBM) for x in arrays]


def whole(space):
    return pl.BlockSpec(memory_space=space)


def params():
    return pltpu.CompilerParams(vmem_limit_bytes=LIMIT)


def cost(flops, size, exps=0):
    return pl.CostEstimate(flops=flops, bytes_accessed=size, transcendentals=exps)


def early_of(order_ref, slot):
    return jnp.minimum(order_ref[2 * slot], order_ref[2 * slot + 1])


def flip_of(order_ref):
    me = lax.axis_index("seq")
    return (order_ref[2 * me] > order_ref[2 * me + 1]).astype(jnp.int32)


def half(index, rows):
    return pl.ds(pl.multiple_of(index * rows, rows), rows)


def split_kernel(order_hbm, k_hbm, v_hbm, early_ref, late_ref, marks_ref, order_ref, kv, sems):
    rows = early_ref.shape[0]
    width = k_hbm.shape[1]
    copies = [
        pltpu.make_async_copy(order_hbm, order_ref, sems.at[0]),
        pltpu.make_async_copy(k_hbm, kv.at[0], sems.at[1]),
        pltpu.make_async_copy(v_hbm, kv.at[1], sems.at[2]),
    ]
    for copy in copies:
        copy.start()
    copies[0].wait()
    me = lax.axis_index("seq")
    mine = early_of(order_ref, me)
    flip = flip_of(order_ref)
    peers = [early_of(order_ref, me ^ p) for p in (1, 2, 3)]
    values = [flip.astype(jnp.float32)]
    values += [jnp.where(c < mine, 0.0, FAR) for c in peers]
    values += [jnp.where(c > mine, 0.0, FAR) for c in peers]
    row = lax.broadcasted_iota(jnp.int32, marks_ref.shape, 0)
    marks = jnp.zeros(marks_ref.shape, jnp.float32)
    for i, value in enumerate(values):
        marks = jnp.where(row == i, value, marks)
    marks_ref[...] = marks
    for i, copy in enumerate(copies[1:]):
        copy.wait()
        lanes = slice(i * width, (i + 1) * width)
        early_ref[:, lanes] = kv[i, half(flip, rows), :]
        late_ref[:, lanes] = kv[i, half(1 - flip, rows), :]


def split_halves(order, keys, values):
    rows, width = keys.shape[0] // 2, keys.shape[1]
    out = vmem_out((rows, 2 * width), keys.dtype)
    return pl.pallas_call(
        split_kernel,
        out_shape=(out, out, vmem_out((8, HEAD_SIZE), jnp.float32)),
        in_specs=[whole(HBM)] * 3,
        out_specs=(whole(VMEM),) * 3,
        scratch_shapes=[
            SMEM(order.shape, order.dtype),
            VMEM((2,) + keys.shape, keys.dtype),
            pltpu.SemaphoreType.DMA((3,)),
        ],
        compiler_params=params(),
        name="split_halves",
        cost_estimate=cost(1000, 1 << 20),
    )(*in_hbm(order, keys, values))


def prep_kernel(order_hbm, w_hbm, q_hbm, r_hbm, w_ref, qe_ref, ql_ref, re_ref, rl_ref, order_ref, sems):
    rows = qe_ref.shape[0]
    first = pltpu.make_async_copy(order_hbm, order_ref, sems.at[0])
    first.start()
    copies = [pltpu.make_async_copy(w_hbm, w_ref, sems.at[1])]
    copies[0].start()
    first.wait()
    flip = flip_of(order_ref)
    pairs = ((q_hbm, qe_ref, flip), (r_hbm, re_ref, flip), (q_hbm, ql_ref, 1 - flip), (r_hbm, rl_ref, 1 - flip))
    for i, (source, target, index) in enumerate(pairs):
        copy = pltpu.make_async_copy(source.at[half(index, rows), :], target, sems.at[2 + i])
        copy.start()
        copies.append(copy)
    for copy in copies:
        copy.wait()


def prep(order, weight, queries, residual):
    rows, cols = queries.shape[0] // 2, queries.shape[1]
    part = vmem_out((rows, cols), queries.dtype)
    other = vmem_out((rows, residual.shape[1]), residual.dtype)
    return pl.pallas_call(
        prep_kernel,
        out_shape=(vmem_out(weight.shape, weight.dtype), part, part, other, other),
        in_specs=[whole(HBM)] * 4,
        out_specs=(whole(VMEM),) * 5,
        scratch_shapes=[SMEM(order.shape, order.dtype), pltpu.SemaphoreType.DMA((6,))],
        compiler_params=pltpu.CompilerParams(vmem_limit_bytes=16 * 2**20),
        name="prep",
        cost_estimate=cost(1 << 26, 16 << 20),
    )(*in_hbm(order, weight, queries, residual))


def attend(q_rows, pieces, biases, diagonal, kv_heads):
    rows = q_rows.shape[0]
    width = kv_heads * HEAD_SIZE
    group = q_rows.shape[1] // width
    factor = HEAD_SIZE ** (-0.5) * math.log2(math.e)
    outs = []
    for h in range(kv_heads):
        lanes = slice(h * HEAD_SIZE, (h + 1) * HEAD_SIZE)
        v_lanes = slice(width + h * HEAD_SIZE, width + (h + 1) * HEAD_SIZE)
        keys = jnp.concatenate([p[:, lanes] for p in pieces], axis=0)
        vals = jnp.concatenate([p[:, v_lanes] for p in pieces], axis=0)
        heads = [
            q_rows[:, (h * group + g) * HEAD_SIZE : (h * group + g + 1) * HEAD_SIZE]
            for g in range(group)
        ]
        stacked = jnp.concatenate(heads, axis=0)
        scores = lax.dot_general(
            stacked, keys, (((1,), (1,)), ((), ())), preferred_element_type=jnp.float32
        )
        parts = []
        for j, bias in enumerate(biases):
            part = scores[:, j * rows : (j + 1) * rows]
            if bias is not None:
                part = part + bias
            parts.append(part)
        last = scores[:, len(biases) * rows :].reshape(group, rows, rows)
        parts.append(jnp.where(diagonal[None], last, FAR).reshape(group * rows, rows))
        peak = functools.reduce(jnp.maximum, parts)
        peak = jnp.max(peak, axis=1, keepdims=True)
        weights = [jnp.exp2((part - peak) * factor) for part in parts]
        total = jnp.sum(functools.reduce(jnp.add, weights), axis=1, keepdims=True)
        rounded = jnp.concatenate([w.astype(jnp.bfloat16) for w in weights], axis=1)
        mixed = lax.dot_general(
            rounded, vals, (((1,), (0,)), ((), ())), preferred_element_type=jnp.float32
        )
        mixed = (mixed / total).astype(jnp.bfloat16)
        outs += [mixed[g * rows : (g + 1) * rows] for g in range(group)]
    return jnp.concatenate(outs, axis=1)


def project(att, w_ref, away_ref, keep_ref, n_core):
    head = lax.axis_index("head")
    chip, core = head // n_core, head % n_core
    cols = away_ref.shape[1] // 2
    for i, owner_chip in enumerate((1 - chip, chip)):
        for ref, owner_core in ((away_ref, 1 - core), (keep_ref, core)):
            start = pl.multiple_of((owner_chip * n_core + owner_core) * cols, cols)
            block = jnp.dot(att, w_ref[:, pl.ds(start, cols)], preferred_element_type=jnp.float32)
            ref[:, i * cols : (i + 1) * cols] = block.astype(ref.dtype)


def side_kernel(late, kv_heads, n_core, marks_ref, q_ref, w_ref, *refs):
    *piece_refs, away_ref, keep_ref = refs
    rows = away_ref.shape[0]
    if late:
        biases = [None] * 4 + [marks_ref[i : i + 1, :] for i in (4, 5, 6)]
    else:
        biases = [marks_ref[i : i + 1, :] for i in (1, 2, 3)]
    row = lax.broadcasted_iota(jnp.int32, (rows, rows), 0)
    col = lax.broadcasted_iota(jnp.int32, (rows, rows), 1)
    att = attend(q_ref[...], [r[...] for r in piece_refs], biases, col <= row, kv_heads)
    project(att, w_ref, away_ref, keep_ref, n_core)


def side(late, kv_heads, n_core, marks, queries, weight, pieces):
    rows, depth = queries.shape
    cols = weight.shape[1] // 2
    keys = rows * len(pieces)
    flops = 4 * rows * depth * keys + 2 * rows * depth * weight.shape[1]
    return pl.pallas_call(
        functools.partial(side_kernel, late, kv_heads, n_core),
        out_shape=(
            vmem_out((rows, cols), jnp.bfloat16),
            vmem_out((rows, cols), jnp.float32),
        ),
        in_specs=[whole(VMEM)] * (3 + len(pieces)),
        out_specs=(whole(VMEM), whole(VMEM)),
        compiler_params=params(),
        name="late_side" if late else "early_side",
        cost_estimate=cost(flops, 16 << 20, rows * depth * keys // HEAD_SIZE),
    )(marks, queries, weight, *pieces)


def mix_kernel(res_ref, keep_ref, core_ref, chip_ref, mixed_ref, sq_ref):
    rows, cols = mixed_ref.shape
    own = keep_ref[:, cols:] + core_ref[:, cols:].astype(jnp.float32)
    mixed = res_ref[...].astype(jnp.float32) + (own + chip_ref[...].astype(jnp.float32))
    mixed_ref[...] = mixed
    squares = mixed * mixed
    lanes = functools.reduce(
        jnp.add, [squares[:, j : j + rows] for j in range(0, cols, rows)]
    )
    sq_ref[...] = jnp.broadcast_to(jnp.sum(lanes.T, axis=0, keepdims=True), sq_ref.shape)


def mix(late, residual, keep, core, chip):
    rows, cols = residual.shape
    return pl.pallas_call(
        mix_kernel,
        out_shape=(vmem_out((rows, cols), jnp.float32), vmem_out((8, rows), jnp.float32)),
        in_specs=[whole(VMEM)] * 4,
        out_specs=(whole(VMEM), whole(VMEM)),
        compiler_params=params(),
        name="late_mix" if late else "early_mix",
        cost_estimate=cost(1 << 20, 2 << 20),
    )(residual, keep, core, chip)


def normed_block(features, mixed_ref, gain, own_ref, other_ref, lanes):
    rows = mixed_ref.shape[0]
    totals = own_ref[0:1] + other_ref[0:1]
    inverse = lax.rsqrt(totals / features + norm_epsilon)
    inverse = jnp.broadcast_to(inverse, (rows, rows)).T
    return mixed_ref[:, lanes] * inverse * gain[:, lanes]


def norm_kernel(features, gain_ref, mixed_ref, own_ref, other_ref, out_ref):
    rows, cols = mixed_ref.shape
    gain = gain_ref[...].astype(jnp.float32)
    for j in range(0, cols, rows):
        lanes = slice(j, j + rows)
        block = normed_block(features, mixed_ref, gain, own_ref, other_ref, lanes)
        out_ref[:, lanes] = block.astype(out_ref.dtype)


def early_norm(features, gain, mixed, own, other):
    return pl.pallas_call(
        functools.partial(norm_kernel, features),
        out_shape=vmem_out(mixed.shape, jnp.bfloat16),
        in_specs=[whole(VMEM)] * 4,
        out_specs=whole(VMEM),
        compiler_params=params(),
        name="early_norm",
        cost_estimate=cost(1 << 20, 1 << 20),
    )(gain, mixed, own, other)


def last_kernel(features, marks_ref, gain_ref, early_ref, mixed_ref, own_ref, other_ref, out_ref):
    rows, cols = mixed_ref.shape
    gain = gain_ref[...].astype(jnp.float32)
    flip = marks_ref[0:1, :] > 0.5
    for j in range(0, cols, rows):
        lanes = slice(j, j + rows)
        late = normed_block(features, mixed_ref, gain, own_ref, other_ref, lanes)
        early = early_ref[:, lanes].astype(jnp.float32)
        out_ref[:rows, lanes] = jnp.where(flip, late, early).astype(out_ref.dtype)
        out_ref[rows:, lanes] = jnp.where(flip, early, late).astype(out_ref.dtype)


def late_norm(features, marks, gain, early, mixed, own, other):
    rows, cols = mixed.shape
    return pl.pallas_call(
        functools.partial(last_kernel, features),
        out_shape=jax.ShapeDtypeStruct((2 * rows, cols), jnp.bfloat16),
        in_specs=[whole(VMEM)] * 6,
        out_specs=whole(VMEM),
        compiler_params=params(),
        name="late_norm",
        cost_estimate=cost(1 << 20, 2 << 20),
    )(marks, gain, early, mixed, own, other)


def paired_body(n_seq, n_head, n_core, *args):
    return paired_steps(n_seq, n_head, n_core, *args)


def paired_steps(n_seq, n_head, n_core, queries, keys, values, residual, weight, gain, order):
    kv_heads = keys.shape[1] // HEAD_SIZE
    cols = residual.shape[1]
    features = n_head * cols

    def send(x, axis, step):
        size = n_seq if axis == "seq" else n_head
        return lax.ppermute(x, axis, [(i, i ^ step) for i in range(size)])

    early, late, marks = split_halves(order, keys, values)
    early_b = send(early, "seq", 2)
    early_a = send(early, "seq", 1)
    late_b = send(late, "seq", 2)
    early_c = send(early_b, "seq", 1)
    late_a = send(late, "seq", 1)
    late_c = send(late_b, "seq", 1)
    held, q_e, q_l, res_e, res_l = prep(order, weight, queries, residual)
    row_gain = gain.reshape(1, cols)

    def chip_share(keep, core):
        return (keep[:, :cols] + core[:, :cols].astype(jnp.float32)).astype(jnp.bfloat16)

    pieces = [early_a, early_b, early_c, early]
    away_e, keep_e = side(False, kv_heads, n_core, marks, q_e, held, pieces)
    core_e = send(away_e, "head", 1)
    chip_e = send(chip_share(keep_e, core_e), "head", n_core)

    pieces = [early, early_a, early_b, early_c, late_a, late_b, late_c, late]
    away_l, keep_l = side(True, kv_heads, n_core, marks, q_l, held, pieces)
    core_l = send(away_l, "head", 1)
    chip_l = send(chip_share(keep_l, core_l), "head", n_core)

    mixed_e, sq_e = mix(False, res_e, keep_e, core_e, chip_e)
    sum_e = sq_e + send(sq_e, "head", 1)
    other_e = send(sum_e, "head", n_core)
    mixed_l, sq_l = mix(True, res_l, keep_l, core_l, chip_l)
    sum_l = sq_l + send(sq_l, "head", 1)
    other_l = send(sum_l, "head", n_core)
    normed_e = early_norm(features, row_gain, mixed_e, sum_e, other_e)
    return late_norm(features, marks, row_gain, normed_e, mixed_l, sum_l, other_l)


def slot_positions(row_ids, block_order, block_rows):
    slot_index = row_ids // block_rows
    slot_ids = jnp.arange(block_order.shape[0], dtype=jnp.int32)
    starts = jnp.sum(
        jnp.where(slot_index[:, None] == slot_ids[None, :], block_order[None, :], 0), axis=1
    )
    return starts * block_rows + row_ids % block_rows


def attend_block(carried, query_rows, query_positions, key_block, value_block, key_positions):
    row_peak, denominators, weighted_sum = carried
    scores = jnp.einsum(
        "qhgd,khd->hgqk", query_rows, key_block, preferred_element_type=jnp.float32
    ) * HEAD_SIZE ** (-0.5)
    visible = (key_positions[None, :] <= query_positions[:, None])[None, None]
    scores = jnp.where(visible, scores, FAR)
    new_peak = jnp.maximum(row_peak, jnp.max(scores, axis=3))
    weights = jnp.where(visible, jnp.exp(scores - new_peak[..., None]), 0.0)
    factor = jnp.exp(row_peak - new_peak)
    denominators = denominators * factor + jnp.sum(weights, axis=3)
    weighted_sum = weighted_sum * factor[..., None] + jnp.einsum(
        "hgqk,khd->hgqd",
        weights.astype(jnp.bfloat16),
        value_block,
        preferred_element_type=jnp.float32,
    )
    return (new_peak, denominators, weighted_sum)


def gathered_body(n_head, queries, keys, values, residual, weight, gain, order):
    tok_rows = queries.shape[0]
    block_rows = tok_rows // 2
    kv_heads = keys.shape[1] // HEAD_SIZE
    q_heads = queries.shape[1] // HEAD_SIZE
    group = q_heads // kv_heads
    own_rows = lax.axis_index("seq") * tok_rows + jnp.arange(tok_rows, dtype=jnp.int32)
    own_positions = slot_positions(own_rows, order, block_rows)
    shaped = queries.reshape(tok_rows, kv_heads, group, HEAD_SIZE)
    all_keys = lax.all_gather(keys, "seq", axis=0, tiled=True)
    all_values = lax.all_gather(values, "seq", axis=0, tiled=True)
    count = all_keys.shape[0]
    width = math.gcd(count, 512)
    all_keys = all_keys.reshape(count, kv_heads, HEAD_SIZE)
    all_values = all_values.reshape(count, kv_heads, HEAD_SIZE)

    def one_step(index, state):
        offset = index * width
        row_ids = offset + jnp.arange(width, dtype=jnp.int32)
        return attend_block(
            state,
            shaped,
            own_positions,
            lax.dynamic_slice_in_dim(all_keys, offset, width, 0),
            lax.dynamic_slice_in_dim(all_values, offset, width, 0),
            slot_positions(row_ids, order, block_rows),
        )

    state = (
        jnp.full((kv_heads, group, tok_rows), FAR, jnp.float32),
        jnp.zeros((kv_heads, group, tok_rows), jnp.float32),
        jnp.zeros((kv_heads, group, tok_rows, HEAD_SIZE), jnp.float32),
    )
    _, denominators, weighted_sum = lax.fori_loop(0, count // width, one_step, state)
    att = (weighted_sum / denominators[..., None]).transpose(2, 0, 1, 3)
    att = att.reshape(tok_rows, q_heads * HEAD_SIZE).astype(jnp.bfloat16)
    partial_terms = jnp.dot(att, weight, preferred_element_type=jnp.float32)
    projected = lax.psum_scatter(
        partial_terms.astype(jnp.bfloat16), "head", scatter_dimension=1, tiled=True
    ).astype(jnp.float32)
    mixed = residual.astype(jnp.float32) + projected
    totals = lax.psum(jnp.sum(mixed * mixed, axis=1), "head")
    inverse = lax.rsqrt(totals / (n_head * residual.shape[1]) + norm_epsilon)
    return (mixed * inverse[:, None] * gain.astype(jnp.float32)[None, :]).astype(jnp.bfloat16)


def solution(mesh):
    n_seq, n_head = mesh.shape["seq"], mesh.shape["head"]
    rows, wide = P(("rep", "seq"), "head"), P("head", None)
    in_specs = (rows, rows, rows, rows, wide, P("head"), P("rep"))
    if n_seq == 4 and n_head == 4:
        body = functools.partial(paired_body, n_seq, n_head, n_head // 2)
    else:
        body = functools.partial(gathered_body, n_head)
    return jax.shard_map(body, mesh=mesh, in_specs=in_specs, out_specs=rows, check_vma=False)
```

```python
import functools
import math

import jax
import jax.numpy as jnp
from jax import lax
from jax.experimental import pallas as pl
from jax.experimental.pallas import tpu as pltpu
from jax.sharding import PartitionSpec as P


HEAD_SIZE = 128
norm_epsilon = 1e-05
FAR = -1e30
VMEM = pltpu.VMEM
SMEM = pltpu.SMEM
HBM = pltpu.HBM
LIMIT = 40 * 2**20


def vmem_out(shape, dtype):
    return pltpu.VMEM(shape, dtype)


def in_hbm(*arrays):
    return [pltpu.with_memory_space_constraint(x, HBM) for x in arrays]


def whole(space):
    return pl.BlockSpec(memory_space=space)


def params():
    return pltpu.CompilerParams(vmem_limit_bytes=LIMIT)


def cost(flops, size, exps=0):
    return pl.CostEstimate(flops=flops, bytes_accessed=size, transcendentals=exps)


def early_of(order_ref, slot):
    return jnp.minimum(order_ref[2 * slot], order_ref[2 * slot + 1])


def flip_of(order_ref):
    me = lax.axis_index("seq")
    return (order_ref[2 * me] > order_ref[2 * me + 1]).astype(jnp.int32)


def half(index, rows):
    return pl.ds(pl.multiple_of(index * rows, rows), rows)


def split_kernel(order_hbm, k_hbm, v_hbm, early_ref, late_ref, marks_ref, order_ref, kv, sems):
    rows = early_ref.shape[0]
    width = k_hbm.shape[1]
    copies = [
        pltpu.make_async_copy(order_hbm, order_ref, sems.at[0]),
        pltpu.make_async_copy(k_hbm, kv.at[0], sems.at[1]),
        pltpu.make_async_copy(v_hbm, kv.at[1], sems.at[2]),
    ]
    for copy in copies:
        copy.start()
    copies[0].wait()
    me = lax.axis_index("seq")
    mine = early_of(order_ref, me)
    flip = flip_of(order_ref)
    peers = [early_of(order_ref, me ^ p) for p in (1, 2, 3)]
    values = [flip.astype(jnp.float32)]
    values += [jnp.where(c < mine, 0.0, FAR) for c in peers]
    values += [jnp.where(c > mine, 0.0, FAR) for c in peers]
    row = lax.broadcasted_iota(jnp.int32, marks_ref.shape, 0)
    marks = jnp.zeros(marks_ref.shape, jnp.float32)
    for i, value in enumerate(values):
        marks = jnp.where(row == i, value, marks)
    marks_ref[...] = marks
    for i, copy in enumerate(copies[1:]):
        copy.wait()
        lanes = slice(i * width, (i + 1) * width)
        early_ref[:, lanes] = kv[i, half(flip, rows), :]
        late_ref[:, lanes] = kv[i, half(1 - flip, rows), :]


def split_halves(order, keys, values):
    rows, width = keys.shape[0] // 2, keys.shape[1]
    out = vmem_out((rows, 2 * width), keys.dtype)
    return pl.pallas_call(
        split_kernel,
        out_shape=(out, out, vmem_out((8, HEAD_SIZE), jnp.float32)),
        in_specs=[whole(HBM)] * 3,
        out_specs=(whole(VMEM),) * 3,
        scratch_shapes=[
            SMEM(order.shape, order.dtype),
            VMEM((2,) + keys.shape, keys.dtype),
            pltpu.SemaphoreType.DMA((3,)),
        ],
        compiler_params=params(),
        name="split_halves",
        cost_estimate=cost(1000, 1 << 20),
    )(*in_hbm(order, keys, values))


def prep_kernel(order_hbm, w_hbm, q_hbm, r_hbm, w_ref, qe_ref, ql_ref, re_ref, rl_ref, order_ref, sems):
    rows = qe_ref.shape[0]
    first = pltpu.make_async_copy(order_hbm, order_ref, sems.at[0])
    first.start()
    copies = [pltpu.make_async_copy(w_hbm, w_ref, sems.at[1])]
    copies[0].start()
    first.wait()
    flip = flip_of(order_ref)
    pairs = ((q_hbm, qe_ref, flip), (r_hbm, re_ref, flip), (q_hbm, ql_ref, 1 - flip), (r_hbm, rl_ref, 1 - flip))
    for i, (source, target, index) in enumerate(pairs):
        copy = pltpu.make_async_copy(source.at[half(index, rows), :], target, sems.at[2 + i])
        copy.start()
        copies.append(copy)
    for copy in copies:
        copy.wait()


def prep(order, weight, queries, residual):
    rows, cols = queries.shape[0] // 2, queries.shape[1]
    part = vmem_out((rows, cols), queries.dtype)
    other = vmem_out((rows, residual.shape[1]), residual.dtype)
    return pl.pallas_call(
        prep_kernel,
        out_shape=(vmem_out(weight.shape, weight.dtype), part, part, other, other),
        in_specs=[whole(HBM)] * 4,
        out_specs=(whole(VMEM),) * 5,
        scratch_shapes=[SMEM(order.shape, order.dtype), pltpu.SemaphoreType.DMA((6,))],
        compiler_params=pltpu.CompilerParams(vmem_limit_bytes=16 * 2**20),
        name="prep",
        cost_estimate=cost(1 << 26, 16 << 20),
    )(*in_hbm(order, weight, queries, residual))


FACTOR = HEAD_SIZE ** (-0.5) * math.log2(math.e)


def head_views(q_rows, pieces, kv_heads):
    width = kv_heads * HEAD_SIZE
    group = q_rows.shape[1] // width
    for h in range(kv_heads):
        lanes = slice(h * HEAD_SIZE, (h + 1) * HEAD_SIZE)
        v_lanes = slice(width + h * HEAD_SIZE, width + (h + 1) * HEAD_SIZE)
        keys = jnp.concatenate([p[:, lanes] for p in pieces], axis=0)
        vals = jnp.concatenate([p[:, v_lanes] for p in pieces], axis=0)
        firsts = [(h * group + g) * HEAD_SIZE for g in range(group)]
        stacked = jnp.concatenate([q_rows[:, f : f + HEAD_SIZE] for f in firsts], axis=0)
        yield stacked, keys, vals


def softmax_terms(stacked, keys, biases, diagonal):
    scores = lax.dot_general(
        stacked, keys, (((1,), (1,)), ((), ())), preferred_element_type=jnp.float32
    )
    rows = keys.shape[0] // (len(biases) + (diagonal is not None))
    parts = []
    for j, bias in enumerate(biases):
        part = scores[:, j * rows : (j + 1) * rows]
        parts.append(part if bias is None else part + bias)
    if diagonal is not None:
        last = scores[:, len(biases) * rows :].reshape(-1, rows, rows)
        parts.append(jnp.where(diagonal[None], last, FAR).reshape(-1, rows))
    peak = jnp.max(functools.reduce(jnp.maximum, parts), axis=1, keepdims=True)
    return parts, peak


def weigh(parts, peak, vals):
    weights = [jnp.exp2((part - peak) * FACTOR) for part in parts]
    total = jnp.sum(functools.reduce(jnp.add, weights), axis=1, keepdims=True)
    rounded = jnp.concatenate([w.astype(jnp.bfloat16) for w in weights], axis=1)
    mixed = lax.dot_general(
        rounded, vals, (((1,), (0,)), ((), ())), preferred_element_type=jnp.float32
    )
    return total, mixed


def unstack(mixed, rows):
    return [mixed[i : i + rows] for i in range(0, mixed.shape[0], rows)]


def lower(rows):
    row = lax.broadcasted_iota(jnp.int32, (rows, rows), 0)
    col = lax.broadcasted_iota(jnp.int32, (rows, rows), 1)
    return col <= row


def first_columns(att, w_ref, away_ref, n_core):
    head = lax.axis_index("head")
    chip, core = head // n_core, head % n_core
    cols = away_ref.shape[1]
    start = pl.multiple_of(((1 - chip) * n_core + 1 - core) * cols, cols)
    block = jnp.dot(att, w_ref[:, pl.ds(start, cols)], preferred_element_type=jnp.float32)
    away_ref[...] = block.astype(away_ref.dtype)


def early_kernel(kv_heads, n_core, marks_ref, q_ref, w_ref, *refs):
    *piece_refs, att_ref, away_ref = refs
    rows = away_ref.shape[0]
    biases = [marks_ref[i : i + 1, :] for i in (1, 2, 3)]
    outs = []
    for stacked, keys, vals in head_views(q_ref[...], [r[...] for r in piece_refs], kv_heads):
        parts, peak = softmax_terms(stacked, keys, biases, lower(rows))
        total, mixed = weigh(parts, peak, vals)
        outs += unstack((mixed / total).astype(jnp.bfloat16), rows)
    att = jnp.concatenate(outs, axis=1)
    att_ref[...] = att
    first_columns(att, w_ref, away_ref, n_core)


def ahead_kernel(kv_heads, q_ref, *refs):
    *piece_refs, peak_ref, total_ref, mixed_ref = refs
    rows = q_ref.shape[0]
    views = head_views(q_ref[...], [r[...] for r in piece_refs], kv_heads)
    for h, (stacked, keys, vals) in enumerate(views):
        parts, peak = softmax_terms(stacked, keys, [None] * 4, lower(rows))
        total, mixed = weigh(parts, peak, vals)
        peak_ref[h] = jnp.broadcast_to(peak, mixed.shape)
        total_ref[h] = jnp.broadcast_to(total, mixed.shape)
        mixed_ref[h] = mixed


def late_kernel(kv_heads, n_core, marks_ref, q_ref, w_ref, peak_ref, total_ref, mixed_ref, *refs):
    *piece_refs, att_ref, away_ref = refs
    rows = away_ref.shape[0]
    biases = [marks_ref[i : i + 1, :] for i in (4, 5, 6)]
    outs = []
    views = head_views(q_ref[...], [r[...] for r in piece_refs], kv_heads)
    for h, (stacked, keys, vals) in enumerate(views):
        parts, peak = softmax_terms(stacked, keys, biases, None)
        before = peak_ref[h]
        peak = jnp.maximum(peak, before)
        factor = jnp.exp2((before - peak) * FACTOR)
        total, mixed = weigh(parts, peak, vals)
        total = total + total_ref[h] * factor
        mixed = mixed + mixed_ref[h] * factor
        outs += unstack((mixed / total).astype(jnp.bfloat16), rows)
    att = jnp.concatenate(outs, axis=1)
    att_ref[...] = att
    first_columns(att, w_ref, away_ref, n_core)


def attend_early(kv_heads, n_core, marks, queries, weight, pieces):
    rows, depth = queries.shape
    cols = weight.shape[1] // (2 * n_core)
    keys = rows * len(pieces)
    return pl.pallas_call(
        functools.partial(early_kernel, kv_heads, n_core),
        out_shape=(vmem_out(queries.shape, jnp.bfloat16), vmem_out((rows, cols), jnp.bfloat16)),
        in_specs=[whole(VMEM)] * (3 + len(pieces)),
        out_specs=(whole(VMEM),) * 2,
        compiler_params=params(),
        name="attend_early",
        cost_estimate=cost(4 * rows * depth * keys + 2 * rows * depth * cols, 4 << 20, 1 << 20),
    )(marks, queries, weight, *pieces)


def attend_ahead(kv_heads, queries, pieces):
    rows, depth = queries.shape
    keys = rows * len(pieces)
    state = vmem_out((kv_heads, rows * depth // (kv_heads * HEAD_SIZE), HEAD_SIZE), jnp.float32)
    return pl.pallas_call(
        functools.partial(ahead_kernel, kv_heads),
        out_shape=(state,) * 3,
        in_specs=[whole(VMEM)] * (1 + len(pieces)),
        out_specs=(whole(VMEM),) * 3,
        compiler_params=params(),
        name="attend_ahead",
        cost_estimate=cost(4 * rows * depth * keys, 4 << 20, 1 << 20),
    )(queries, *pieces)


def attend_late(kv_heads, n_core, marks, queries, weight, state, pieces):
    rows, depth = queries.shape
    cols = weight.shape[1] // (2 * n_core)
    keys = rows * len(pieces)
    return pl.pallas_call(
        functools.partial(late_kernel, kv_heads, n_core),
        out_shape=(vmem_out(queries.shape, jnp.bfloat16), vmem_out((rows, cols), jnp.bfloat16)),
        in_specs=[whole(VMEM)] * (6 + len(pieces)),
        out_specs=(whole(VMEM),) * 2,
        compiler_params=params(),
        name="attend_late",
        cost_estimate=cost(4 * rows * depth * keys + 2 * rows * depth * cols, 4 << 20, 1 << 20),
    )(marks, queries, weight, *state, *pieces)


def rest_kernel(n_core, att_ref, w_ref, share_ref, away_ref, keep_ref):
    head = lax.axis_index("head")
    chip, core = head // n_core, head % n_core
    cols = keep_ref.shape[1]
    owners = ((1 - chip, core, share_ref), (chip, 1 - core, away_ref), (chip, core, keep_ref))
    for owner_chip, owner_core, ref in owners:
        start = pl.multiple_of((owner_chip * n_core + owner_core) * cols, cols)
        block = jnp.dot(
            att_ref[...], w_ref[:, pl.ds(start, cols)], preferred_element_type=jnp.float32
        )
        ref[...] = block.astype(ref.dtype)


def project_rest(late, n_core, att, weight):
    rows, depth = att.shape
    cols = weight.shape[1] // (2 * n_core)
    return pl.pallas_call(
        functools.partial(rest_kernel, n_core),
        out_shape=(
            vmem_out((rows, cols), jnp.float32),
            vmem_out((rows, cols), jnp.bfloat16),
            vmem_out((rows, cols), jnp.float32),
        ),
        in_specs=[whole(VMEM)] * 2,
        out_specs=(whole(VMEM),) * 3,
        compiler_params=params(),
        name="late_rest" if late else "early_rest",
        cost_estimate=cost(6 * rows * depth * cols, 8 << 20),
    )(att, weight)


def mix_kernel(res_ref, keep_ref, core_ref, chip_ref, mixed_ref, sq_ref):
    rows, cols = mixed_ref.shape
    own = keep_ref[...] + core_ref[...].astype(jnp.float32)
    mixed = res_ref[...].astype(jnp.float32) + (own + chip_ref[...].astype(jnp.float32))
    mixed_ref[...] = mixed
    squares = mixed * mixed
    lanes = functools.reduce(
        jnp.add, [squares[:, j : j + rows] for j in range(0, cols, rows)]
    )
    sq_ref[...] = jnp.broadcast_to(jnp.sum(lanes.T, axis=0, keepdims=True), sq_ref.shape)


def mix(late, residual, keep, core, chip):
    rows, cols = residual.shape
    return pl.pallas_call(
        mix_kernel,
        out_shape=(vmem_out((rows, cols), jnp.float32), vmem_out((8, rows), jnp.float32)),
        in_specs=[whole(VMEM)] * 4,
        out_specs=(whole(VMEM), whole(VMEM)),
        compiler_params=params(),
        name="late_mix" if late else "early_mix",
        cost_estimate=cost(1 << 20, 2 << 20),
    )(residual, keep, core, chip)


def normed_block(features, mixed_ref, gain, own_ref, other_ref, lanes):
    rows = mixed_ref.shape[0]
    totals = own_ref[0:1] + other_ref[0:1]
    inverse = lax.rsqrt(totals / features + norm_epsilon)
    inverse = jnp.broadcast_to(inverse, (rows, rows)).T
    return mixed_ref[:, lanes] * inverse * gain[:, lanes]


def norm_kernel(features, gain_ref, mixed_ref, own_ref, other_ref, out_ref):
    rows, cols = mixed_ref.shape
    gain = gain_ref[...].astype(jnp.float32)
    for j in range(0, cols, rows):
        lanes = slice(j, j + rows)
        block = normed_block(features, mixed_ref, gain, own_ref, other_ref, lanes)
        out_ref[:, lanes] = block.astype(out_ref.dtype)


def early_norm(features, gain, mixed, own, other):
    return pl.pallas_call(
        functools.partial(norm_kernel, features),
        out_shape=vmem_out(mixed.shape, jnp.bfloat16),
        in_specs=[whole(VMEM)] * 4,
        out_specs=whole(VMEM),
        compiler_params=params(),
        name="early_norm",
        cost_estimate=cost(1 << 20, 1 << 20),
    )(gain, mixed, own, other)


def last_kernel(features, marks_ref, gain_ref, early_ref, mixed_ref, own_ref, other_ref, out_ref):
    rows, cols = mixed_ref.shape
    gain = gain_ref[...].astype(jnp.float32)
    flip = marks_ref[0:1, :] > 0.5
    for j in range(0, cols, rows):
        lanes = slice(j, j + rows)
        late = normed_block(features, mixed_ref, gain, own_ref, other_ref, lanes)
        early = early_ref[:, lanes].astype(jnp.float32)
        out_ref[:rows, lanes] = jnp.where(flip, late, early).astype(out_ref.dtype)
        out_ref[rows:, lanes] = jnp.where(flip, early, late).astype(out_ref.dtype)


def late_norm(features, marks, gain, early, mixed, own, other):
    rows, cols = mixed.shape
    return pl.pallas_call(
        functools.partial(last_kernel, features),
        out_shape=jax.ShapeDtypeStruct((2 * rows, cols), jnp.bfloat16),
        in_specs=[whole(VMEM)] * 6,
        out_specs=whole(VMEM),
        compiler_params=params(),
        name="late_norm",
        cost_estimate=cost(1 << 20, 2 << 20),
    )(marks, gain, early, mixed, own, other)


def paired_body(n_seq, n_head, n_core, *args):
    return paired_steps(n_seq, n_head, n_core, *args)


def paired_steps(n_seq, n_head, n_core, queries, keys, values, residual, weight, gain, order):
    kv_heads = keys.shape[1] // HEAD_SIZE
    cols = residual.shape[1]
    features = n_head * cols

    def send(x, axis, step):
        size = n_seq if axis == "seq" else n_head
        return lax.ppermute(x, axis, [(i, i ^ step) for i in range(size)])

    early, late, marks = split_halves(order, keys, values)
    early_b = send(early, "seq", 2)
    early_a = send(early, "seq", 1)
    late_b = send(late, "seq", 2)
    early_c = send(early_b, "seq", 1)
    late_a = send(late, "seq", 1)
    late_c = send(late_b, "seq", 1)
    held, q_e, q_l, res_e, res_l = prep(order, weight, queries, residual)
    row_gain = gain.reshape(1, cols)

    def project(att, away, late):
        core = send(away, "head", 1)
        share, away, keep = project_rest(late, n_core, att, held)
        summed = (share + core.astype(jnp.float32)).astype(jnp.bfloat16)
        chip = send(summed, "head", n_core)
        core = send(away, "head", 1)
        return keep, core, chip

    pieces = [early_a, early_b, early_c, early]
    att, away = attend_early(kv_heads, n_core, marks, q_e, held, pieces)
    keep_e, core_e, chip_e = project(att, away, False)

    pieces = [early, early_a, early_b, early_c, late]
    state = attend_ahead(kv_heads, q_l, pieces)
    pieces = [late_a, late_b, late_c]
    att, away = attend_late(kv_heads, n_core, marks, q_l, held, state, pieces)
    keep_l, core_l, chip_l = project(att, away, True)

    mixed_e, sq_e = mix(False, res_e, keep_e, core_e, chip_e)
    sum_e = sq_e + send(sq_e, "head", 1)
    other_e = send(sum_e, "head", n_core)
    mixed_l, sq_l = mix(True, res_l, keep_l, core_l, chip_l)
    sum_l = sq_l + send(sq_l, "head", 1)
    other_l = send(sum_l, "head", n_core)
    normed_e = early_norm(features, row_gain, mixed_e, sum_e, other_e)
    return late_norm(features, marks, row_gain, normed_e, mixed_l, sum_l, other_l)


def slot_positions(row_ids, block_order, block_rows):
    slot_index = row_ids // block_rows
    slot_ids = jnp.arange(block_order.shape[0], dtype=jnp.int32)
    starts = jnp.sum(
        jnp.where(slot_index[:, None] == slot_ids[None, :], block_order[None, :], 0), axis=1
    )
    return starts * block_rows + row_ids % block_rows


def attend_block(carried, query_rows, query_positions, key_block, value_block, key_positions):
    row_peak, denominators, weighted_sum = carried
    scores = jnp.einsum(
        "qhgd,khd->hgqk", query_rows, key_block, preferred_element_type=jnp.float32
    ) * HEAD_SIZE ** (-0.5)
    visible = (key_positions[None, :] <= query_positions[:, None])[None, None]
    scores = jnp.where(visible, scores, FAR)
    new_peak = jnp.maximum(row_peak, jnp.max(scores, axis=3))
    weights = jnp.where(visible, jnp.exp(scores - new_peak[..., None]), 0.0)
    factor = jnp.exp(row_peak - new_peak)
    denominators = denominators * factor + jnp.sum(weights, axis=3)
    weighted_sum = weighted_sum * factor[..., None] + jnp.einsum(
        "hgqk,khd->hgqd",
        weights.astype(jnp.bfloat16),
        value_block,
        preferred_element_type=jnp.float32,
    )
    return (new_peak, denominators, weighted_sum)


def gathered_body(n_head, queries, keys, values, residual, weight, gain, order):
    tok_rows = queries.shape[0]
    block_rows = tok_rows // 2
    kv_heads = keys.shape[1] // HEAD_SIZE
    q_heads = queries.shape[1] // HEAD_SIZE
    group = q_heads // kv_heads
    own_rows = lax.axis_index("seq") * tok_rows + jnp.arange(tok_rows, dtype=jnp.int32)
    own_positions = slot_positions(own_rows, order, block_rows)
    shaped = queries.reshape(tok_rows, kv_heads, group, HEAD_SIZE)
    all_keys = lax.all_gather(keys, "seq", axis=0, tiled=True)
    all_values = lax.all_gather(values, "seq", axis=0, tiled=True)
    count = all_keys.shape[0]
    width = math.gcd(count, 512)
    all_keys = all_keys.reshape(count, kv_heads, HEAD_SIZE)
    all_values = all_values.reshape(count, kv_heads, HEAD_SIZE)

    def one_step(index, state):
        offset = index * width
        row_ids = offset + jnp.arange(width, dtype=jnp.int32)
        return attend_block(
            state,
            shaped,
            own_positions,
            lax.dynamic_slice_in_dim(all_keys, offset, width, 0),
            lax.dynamic_slice_in_dim(all_values, offset, width, 0),
            slot_positions(row_ids, order, block_rows),
        )

    state = (
        jnp.full((kv_heads, group, tok_rows), FAR, jnp.float32),
        jnp.zeros((kv_heads, group, tok_rows), jnp.float32),
        jnp.zeros((kv_heads, group, tok_rows, HEAD_SIZE), jnp.float32),
    )
    _, denominators, weighted_sum = lax.fori_loop(0, count // width, one_step, state)
    att = (weighted_sum / denominators[..., None]).transpose(2, 0, 1, 3)
    att = att.reshape(tok_rows, q_heads * HEAD_SIZE).astype(jnp.bfloat16)
    partial_terms = jnp.dot(att, weight, preferred_element_type=jnp.float32)
    projected = lax.psum_scatter(
        partial_terms.astype(jnp.bfloat16), "head", scatter_dimension=1, tiled=True
    ).astype(jnp.float32)
    mixed = residual.astype(jnp.float32) + projected
    totals = lax.psum(jnp.sum(mixed * mixed, axis=1), "head")
    inverse = lax.rsqrt(totals / (n_head * residual.shape[1]) + norm_epsilon)
    return (mixed * inverse[:, None] * gain.astype(jnp.float32)[None, :]).astype(jnp.bfloat16)


def solution(mesh):
    n_seq, n_head = mesh.shape["seq"], mesh.shape["head"]
    rows, wide = P(("rep", "seq"), "head"), P("head", None)
    in_specs = (rows, rows, rows, rows, wide, P("head"), P("rep"))
    if n_seq == 4 and n_head == 4:
        body = functools.partial(paired_body, n_seq, n_head, n_head // 2)
    else:
        body = functools.partial(gathered_body, n_head)
    return jax.shard_map(body, mesh=mesh, in_specs=in_specs, out_specs=rows, check_vma=False)
```

```python
import functools
import math

import jax
import jax.numpy as jnp
from jax import lax
from jax.experimental import pallas as pl
from jax.experimental.pallas import tpu as pltpu
from jax.sharding import PartitionSpec as P


HEAD_SIZE = 128
norm_epsilon = 1e-05
FAR = -1e30
VMEM = pltpu.VMEM
SMEM = pltpu.SMEM
HBM = pltpu.HBM
LIMIT = 40 * 2**20


def vmem_out(shape, dtype):
    return pltpu.VMEM(shape, dtype)


def in_hbm(*arrays):
    return [pltpu.with_memory_space_constraint(x, HBM) for x in arrays]


def whole(space):
    return pl.BlockSpec(memory_space=space)


def params():
    return pltpu.CompilerParams(vmem_limit_bytes=LIMIT)


def cost(flops, size, exps=0):
    return pl.CostEstimate(flops=flops, bytes_accessed=size, transcendentals=exps)


def early_of(order_ref, slot):
    return jnp.minimum(order_ref[2 * slot], order_ref[2 * slot + 1])


def flip_of(order_ref):
    me = lax.axis_index("seq")
    return (order_ref[2 * me] > order_ref[2 * me + 1]).astype(jnp.int32)


def half(index, rows):
    return pl.ds(pl.multiple_of(index * rows, rows), rows)


def split_kernel(order_hbm, k_hbm, v_hbm, early_ref, late_ref, marks_ref, order_ref, kv, sems):
    rows = early_ref.shape[0]
    width = k_hbm.shape[1]
    copies = [
        pltpu.make_async_copy(order_hbm, order_ref, sems.at[0]),
        pltpu.make_async_copy(k_hbm, kv.at[0], sems.at[1]),
        pltpu.make_async_copy(v_hbm, kv.at[1], sems.at[2]),
    ]
    for copy in copies:
        copy.start()
    copies[0].wait()
    me = lax.axis_index("seq")
    mine = early_of(order_ref, me)
    flip = flip_of(order_ref)
    peers = [early_of(order_ref, me ^ p) for p in (1, 2, 3)]
    values = [flip.astype(jnp.float32)]
    values += [jnp.where(c < mine, 0.0, FAR) for c in peers]
    values += [jnp.where(c > mine, 0.0, FAR) for c in peers]
    row = lax.broadcasted_iota(jnp.int32, marks_ref.shape, 0)
    marks = jnp.zeros(marks_ref.shape, jnp.float32)
    for i, value in enumerate(values):
        marks = jnp.where(row == i, value, marks)
    marks_ref[...] = marks
    for i, copy in enumerate(copies[1:]):
        copy.wait()
        lanes = slice(i * width, (i + 1) * width)
        early_ref[:, lanes] = kv[i, half(flip, rows), :]
        late_ref[:, lanes] = kv[i, half(1 - flip, rows), :]


def split_halves(order, keys, values):
    rows, width = keys.shape[0] // 2, keys.shape[1]
    out = vmem_out((rows, 2 * width), keys.dtype)
    return pl.pallas_call(
        split_kernel,
        out_shape=(out, out, vmem_out((8, HEAD_SIZE), jnp.float32)),
        in_specs=[whole(HBM)] * 3,
        out_specs=(whole(VMEM),) * 3,
        scratch_shapes=[
            SMEM(order.shape, order.dtype),
            VMEM((2,) + keys.shape, keys.dtype),
            pltpu.SemaphoreType.DMA((3,)),
        ],
        compiler_params=params(),
        name="split_halves",
        cost_estimate=cost(1000, 1 << 20),
    )(*in_hbm(order, keys, values))


def prep_kernel(order_hbm, w_hbm, q_hbm, r_hbm, w_ref, qe_ref, ql_ref, re_ref, rl_ref, order_ref, sems):
    rows = qe_ref.shape[0]
    first = pltpu.make_async_copy(order_hbm, order_ref, sems.at[0])
    first.start()
    copies = [pltpu.make_async_copy(w_hbm, w_ref, sems.at[1])]
    copies[0].start()
    first.wait()
    flip = flip_of(order_ref)
    pairs = ((q_hbm, qe_ref, flip), (r_hbm, re_ref, flip), (q_hbm, ql_ref, 1 - flip), (r_hbm, rl_ref, 1 - flip))
    for i, (source, target, index) in enumerate(pairs):
        copy = pltpu.make_async_copy(source.at[half(index, rows), :], target, sems.at[2 + i])
        copy.start()
        copies.append(copy)
    for copy in copies:
        copy.wait()


def prep(order, weight, queries, residual):
    rows, cols = queries.shape[0] // 2, queries.shape[1]
    part = vmem_out((rows, cols), queries.dtype)
    other = vmem_out((rows, residual.shape[1]), residual.dtype)
    return pl.pallas_call(
        prep_kernel,
        out_shape=(vmem_out(weight.shape, weight.dtype), part, part, other, other),
        in_specs=[whole(HBM)] * 4,
        out_specs=(whole(VMEM),) * 5,
        scratch_shapes=[SMEM(order.shape, order.dtype), pltpu.SemaphoreType.DMA((6,))],
        compiler_params=pltpu.CompilerParams(vmem_limit_bytes=16 * 2**20),
        name="prep",
        cost_estimate=cost(1 << 26, 16 << 20),
    )(*in_hbm(order, weight, queries, residual))


FACTOR = HEAD_SIZE ** (-0.5) * math.log2(math.e)


def head_views(q_rows, pieces, kv_heads):
    width = kv_heads * HEAD_SIZE
    group = q_rows.shape[1] // width
    for h in range(kv_heads):
        lanes = slice(h * HEAD_SIZE, (h + 1) * HEAD_SIZE)
        v_lanes = slice(width + h * HEAD_SIZE, width + (h + 1) * HEAD_SIZE)
        keys = jnp.concatenate([p[:, lanes] for p in pieces], axis=0)
        vals = jnp.concatenate([p[:, v_lanes] for p in pieces], axis=0)
        firsts = [(h * group + g) * HEAD_SIZE for g in range(group)]
        stacked = jnp.concatenate([q_rows[:, f : f + HEAD_SIZE] for f in firsts], axis=0)
        yield stacked, keys, vals


def masked_scores(stacked, keys, biases, diagonal):
    scores = lax.dot_general(
        stacked, keys, (((1,), (1,)), ((), ())), preferred_element_type=jnp.float32
    )
    rows = keys.shape[0] // (len(biases) + (diagonal is not None))
    parts = []
    for j, bias in enumerate(biases):
        part = scores[:, j * rows : (j + 1) * rows]
        parts.append(part if bias is None else part + bias)
    if diagonal is not None:
        last = scores[:, len(biases) * rows :].reshape(-1, rows, rows)
        parts.append(jnp.where(diagonal[None], last, FAR).reshape(-1, rows))
    peak = jnp.max(functools.reduce(jnp.maximum, parts), axis=1, keepdims=True)
    return parts, peak


def weigh(parts, peak, vals):
    weights = [jnp.exp2((part - peak) * FACTOR) for part in parts]
    total = jnp.sum(functools.reduce(jnp.add, weights), axis=1, keepdims=True)
    rounded = jnp.concatenate([w.astype(jnp.bfloat16) for w in weights], axis=1)
    mixed = lax.dot_general(
        rounded, vals, (((1,), (0,)), ((), ())), preferred_element_type=jnp.float32
    )
    return total, mixed


def unstack(mixed, rows):
    return [mixed[i : i + rows] for i in range(0, mixed.shape[0], rows)]


def lower(rows):
    row = lax.broadcasted_iota(jnp.int32, (rows, rows), 0)
    col = lax.broadcasted_iota(jnp.int32, (rows, rows), 1)
    return col <= row


def first_columns(att, w_ref, away_ref, n_core):
    head = lax.axis_index("head")
    chip, core = head // n_core, head % n_core
    cols = away_ref.shape[1]
    start = pl.multiple_of(((1 - chip) * n_core + 1 - core) * cols, cols)
    block = jnp.dot(att, w_ref[:, pl.ds(start, cols)], preferred_element_type=jnp.float32)
    away_ref[...] = block.astype(away_ref.dtype)


def ahead_kernel(kv_heads, late, marks_ref, q_ref, *refs):
    *piece_refs, peak_ref, total_ref, mixed_ref = refs
    rows = piece_refs[-1].shape[0]
    biases = [None] * (len(piece_refs) - 1) if late else [marks_ref[i : i + 1, :] for i in (1, 2)]
    views = head_views(q_ref[...], [r[...] for r in piece_refs], kv_heads)
    for h, (stacked, keys, vals) in enumerate(views):
        parts, peak = masked_scores(stacked, keys, biases, lower(rows))
        total, mixed = weigh(parts, peak, vals)
        peak_ref[h] = jnp.broadcast_to(peak, mixed.shape)
        total_ref[h] = jnp.broadcast_to(total, mixed.shape)
        mixed_ref[h] = mixed


def attend_kernel(
    kv_heads, n_core, late, marks_ref, q_ref, w_ref, peak_ref, total_ref, mixed_ref, *refs
):
    *piece_refs, att_ref, away_ref = refs
    rows = away_ref.shape[0]
    biases = [None] * (len(piece_refs) - 3) if late else []
    biases += [marks_ref[i : i + 1, :] for i in ((4, 5, 6) if late else (3,))]
    outs = []
    views = head_views(q_ref[...], [r[...] for r in piece_refs], kv_heads)
    for h, (stacked, keys, vals) in enumerate(views):
        parts, peak = masked_scores(stacked, keys, biases, None)
        before = peak_ref[h]
        peak = jnp.maximum(peak, before)
        factor = jnp.exp2((before - peak) * FACTOR)
        total, mixed = weigh(parts, peak, vals)
        total = total + total_ref[h] * factor
        mixed = mixed + mixed_ref[h] * factor
        outs += unstack((mixed / total).astype(jnp.bfloat16), rows)
    att = jnp.concatenate(outs, axis=1)
    att_ref[...] = att
    first_columns(att, w_ref, away_ref, n_core)


def attend_ahead(kv_heads, late, marks, queries, pieces):
    rows, depth = queries.shape
    keys = rows * len(pieces)
    state = vmem_out((kv_heads, rows * depth // (kv_heads * HEAD_SIZE), HEAD_SIZE), jnp.float32)
    return pl.pallas_call(
        functools.partial(ahead_kernel, kv_heads, late),
        out_shape=(state,) * 3,
        in_specs=[whole(VMEM)] * (2 + len(pieces)),
        out_specs=(whole(VMEM),) * 3,
        compiler_params=params(),
        name="late_ahead" if late else "early_ahead",
        cost_estimate=cost(4 * rows * depth * keys, 4 << 20, 1 << 20),
    )(marks, queries, *pieces)


def attend(kv_heads, n_core, late, marks, queries, weight, state, pieces):
    rows, depth = queries.shape
    cols = weight.shape[1] // (2 * n_core)
    keys = rows * len(pieces)
    return pl.pallas_call(
        functools.partial(attend_kernel, kv_heads, n_core, late),
        out_shape=(vmem_out(queries.shape, jnp.bfloat16), vmem_out((rows, cols), jnp.bfloat16)),
        in_specs=[whole(VMEM)] * (6 + len(pieces)),
        out_specs=(whole(VMEM),) * 2,
        compiler_params=params(),
        name="attend_late" if late else "attend_early",
        cost_estimate=cost(4 * rows * depth * keys + 2 * rows * depth * cols, 4 << 20, 1 << 20),
    )(marks, queries, weight, *state, *pieces)


def rest_kernel(n_core, att_ref, w_ref, share_ref, away_ref, keep_ref):
    head = lax.axis_index("head")
    chip, core = head // n_core, head % n_core
    cols = keep_ref.shape[1]
    owners = ((1 - chip, core, share_ref), (chip, 1 - core, away_ref), (chip, core, keep_ref))
    for owner_chip, owner_core, ref in owners:
        start = pl.multiple_of((owner_chip * n_core + owner_core) * cols, cols)
        block = jnp.dot(
            att_ref[...], w_ref[:, pl.ds(start, cols)], preferred_element_type=jnp.float32
        )
        ref[...] = block.astype(ref.dtype)


def project_rest(late, n_core, att, weight):
    rows, depth = att.shape
    cols = weight.shape[1] // (2 * n_core)
    return pl.pallas_call(
        functools.partial(rest_kernel, n_core),
        out_shape=(
            vmem_out((rows, cols), jnp.float32),
            vmem_out((rows, cols), jnp.bfloat16),
            vmem_out((rows, cols), jnp.float32),
        ),
        in_specs=[whole(VMEM)] * 2,
        out_specs=(whole(VMEM),) * 3,
        compiler_params=params(),
        name="late_rest" if late else "early_rest",
        cost_estimate=cost(6 * rows * depth * cols, 8 << 20),
    )(att, weight)


def mix_kernel(res_ref, keep_ref, core_ref, chip_ref, mixed_ref, sq_ref):
    rows, cols = mixed_ref.shape
    own = keep_ref[...] + core_ref[...].astype(jnp.float32)
    mixed = res_ref[...].astype(jnp.float32) + (own + chip_ref[...].astype(jnp.float32))
    mixed_ref[...] = mixed
    squares = mixed * mixed
    lanes = functools.reduce(
        jnp.add, [squares[:, j : j + rows] for j in range(0, cols, rows)]
    )
    sq_ref[...] = jnp.broadcast_to(jnp.sum(lanes.T, axis=0, keepdims=True), sq_ref.shape)


def mix(late, residual, keep, core, chip):
    rows, cols = residual.shape
    return pl.pallas_call(
        mix_kernel,
        out_shape=(vmem_out((rows, cols), jnp.float32), vmem_out((8, rows), jnp.float32)),
        in_specs=[whole(VMEM)] * 4,
        out_specs=(whole(VMEM), whole(VMEM)),
        compiler_params=params(),
        name="late_mix" if late else "early_mix",
        cost_estimate=cost(1 << 20, 2 << 20),
    )(residual, keep, core, chip)


def normed_block(features, mixed_ref, gain, own_ref, other_ref, lanes):
    rows = mixed_ref.shape[0]
    totals = own_ref[0:1] + other_ref[0:1]
    inverse = lax.rsqrt(totals / features + norm_epsilon)
    inverse = jnp.broadcast_to(inverse, (rows, rows)).T
    return mixed_ref[:, lanes] * inverse * gain[:, lanes]


def norm_kernel(features, gain_ref, mixed_ref, own_ref, other_ref, out_ref):
    rows, cols = mixed_ref.shape
    gain = gain_ref[...].astype(jnp.float32)
    for j in range(0, cols, rows):
        lanes = slice(j, j + rows)
        block = normed_block(features, mixed_ref, gain, own_ref, other_ref, lanes)
        out_ref[:, lanes] = block.astype(out_ref.dtype)


def early_norm(features, gain, mixed, own, other):
    return pl.pallas_call(
        functools.partial(norm_kernel, features),
        out_shape=vmem_out(mixed.shape, jnp.bfloat16),
        in_specs=[whole(VMEM)] * 4,
        out_specs=whole(VMEM),
        compiler_params=params(),
        name="early_norm",
        cost_estimate=cost(1 << 20, 1 << 20),
    )(gain, mixed, own, other)


def last_kernel(features, marks_ref, gain_ref, early_ref, mixed_ref, own_ref, other_ref, out_ref):
    rows, cols = mixed_ref.shape
    gain = gain_ref[...].astype(jnp.float32)
    flip = marks_ref[0:1, :] > 0.5
    for j in range(0, cols, rows):
        lanes = slice(j, j + rows)
        late = normed_block(features, mixed_ref, gain, own_ref, other_ref, lanes)
        early = early_ref[:, lanes].astype(jnp.float32)
        out_ref[:rows, lanes] = jnp.where(flip, late, early).astype(out_ref.dtype)
        out_ref[rows:, lanes] = jnp.where(flip, early, late).astype(out_ref.dtype)


def late_norm(features, marks, gain, early, mixed, own, other):
    rows, cols = mixed.shape
    return pl.pallas_call(
        functools.partial(last_kernel, features),
        out_shape=jax.ShapeDtypeStruct((2 * rows, cols), jnp.bfloat16),
        in_specs=[whole(VMEM)] * 6,
        out_specs=whole(VMEM),
        compiler_params=params(),
        name="late_norm",
        cost_estimate=cost(1 << 20, 2 << 20),
    )(marks, gain, early, mixed, own, other)


def paired_body(n_seq, n_head, n_core, *args):
    return paired_steps(n_seq, n_head, n_core, *args)


def paired_steps(n_seq, n_head, n_core, queries, keys, values, residual, weight, gain, order):
    kv_heads = keys.shape[1] // HEAD_SIZE
    cols = residual.shape[1]
    features = n_head * cols

    def send(x, axis, step):
        size = n_seq if axis == "seq" else n_head
        return lax.ppermute(x, axis, [(i, i ^ step) for i in range(size)])

    early, late, marks = split_halves(order, keys, values)
    early_b = send(early, "seq", 2)
    early_a = send(early, "seq", 1)
    late_b = send(late, "seq", 2)
    early_c = send(early_b, "seq", 1)
    late_a = send(late, "seq", 1)
    late_c = send(late_b, "seq", 1)
    held, q_e, q_l, res_e, res_l = prep(order, weight, queries, residual)
    row_gain = gain.reshape(1, cols)

    def project(att, away, late):
        core = send(away, "head", 1)
        share, away, keep = project_rest(late, n_core, att, held)
        summed = (share + core.astype(jnp.float32)).astype(jnp.bfloat16)
        chip = send(summed, "head", n_core)
        core = send(away, "head", 1)
        return keep, core, chip

    pieces = [early_a, early_b, early]
    state_e = attend_ahead(kv_heads, False, marks, q_e, pieces)
    pieces = [early, early_a, early_b, late]
    state_l = attend_ahead(kv_heads, True, marks, q_l, pieces)
    att, away = attend(kv_heads, n_core, False, marks, q_e, held, state_e, [early_c])
    keep_e, core_e, chip_e = project(att, away, False)

    pieces = [early_c, late_a, late_b, late_c]
    att, away = attend(kv_heads, n_core, True, marks, q_l, held, state_l, pieces)
    keep_l, core_l, chip_l = project(att, away, True)

    mixed_e, sq_e = mix(False, res_e, keep_e, core_e, chip_e)
    sum_e = sq_e + send(sq_e, "head", 1)
    other_e = send(sum_e, "head", n_core)
    mixed_l, sq_l = mix(True, res_l, keep_l, core_l, chip_l)
    sum_l = sq_l + send(sq_l, "head", 1)
    other_l = send(sum_l, "head", n_core)
    normed_e = early_norm(features, row_gain, mixed_e, sum_e, other_e)
    return late_norm(features, marks, row_gain, normed_e, mixed_l, sum_l, other_l)


def slot_positions(row_ids, block_order, block_rows):
    slot_index = row_ids // block_rows
    slot_ids = jnp.arange(block_order.shape[0], dtype=jnp.int32)
    starts = jnp.sum(
        jnp.where(slot_index[:, None] == slot_ids[None, :], block_order[None, :], 0), axis=1
    )
    return starts * block_rows + row_ids % block_rows


def attend_block(carried, query_rows, query_positions, key_block, value_block, key_positions):
    row_peak, denominators, weighted_sum = carried
    scores = jnp.einsum(
        "qhgd,khd->hgqk", query_rows, key_block, preferred_element_type=jnp.float32
    ) * HEAD_SIZE ** (-0.5)
    visible = (key_positions[None, :] <= query_positions[:, None])[None, None]
    scores = jnp.where(visible, scores, FAR)
    new_peak = jnp.maximum(row_peak, jnp.max(scores, axis=3))
    weights = jnp.where(visible, jnp.exp(scores - new_peak[..., None]), 0.0)
    factor = jnp.exp(row_peak - new_peak)
    denominators = denominators * factor + jnp.sum(weights, axis=3)
    weighted_sum = weighted_sum * factor[..., None] + jnp.einsum(
        "hgqk,khd->hgqd",
        weights.astype(jnp.bfloat16),
        value_block,
        preferred_element_type=jnp.float32,
    )
    return (new_peak, denominators, weighted_sum)


def gathered_body(n_head, queries, keys, values, residual, weight, gain, order):
    tok_rows = queries.shape[0]
    block_rows = tok_rows // 2
    kv_heads = keys.shape[1] // HEAD_SIZE
    q_heads = queries.shape[1] // HEAD_SIZE
    group = q_heads // kv_heads
    own_rows = lax.axis_index("seq") * tok_rows + jnp.arange(tok_rows, dtype=jnp.int32)
    own_positions = slot_positions(own_rows, order, block_rows)
    shaped = queries.reshape(tok_rows, kv_heads, group, HEAD_SIZE)
    all_keys = lax.all_gather(keys, "seq", axis=0, tiled=True)
    all_values = lax.all_gather(values, "seq", axis=0, tiled=True)
    count = all_keys.shape[0]
    width = math.gcd(count, 512)
    all_keys = all_keys.reshape(count, kv_heads, HEAD_SIZE)
    all_values = all_values.reshape(count, kv_heads, HEAD_SIZE)

    def one_step(index, state):
        offset = index * width
        row_ids = offset + jnp.arange(width, dtype=jnp.int32)
        return attend_block(
            state,
            shaped,
            own_positions,
            lax.dynamic_slice_in_dim(all_keys, offset, width, 0),
            lax.dynamic_slice_in_dim(all_values, offset, width, 0),
            slot_positions(row_ids, order, block_rows),
        )

    state = (
        jnp.full((kv_heads, group, tok_rows), FAR, jnp.float32),
        jnp.zeros((kv_heads, group, tok_rows), jnp.float32),
        jnp.zeros((kv_heads, group, tok_rows, HEAD_SIZE), jnp.float32),
    )
    _, denominators, weighted_sum = lax.fori_loop(0, count // width, one_step, state)
    att = (weighted_sum / denominators[..., None]).transpose(2, 0, 1, 3)
    att = att.reshape(tok_rows, q_heads * HEAD_SIZE).astype(jnp.bfloat16)
    partial_terms = jnp.dot(att, weight, preferred_element_type=jnp.float32)
    projected = lax.psum_scatter(
        partial_terms.astype(jnp.bfloat16), "head", scatter_dimension=1, tiled=True
    ).astype(jnp.float32)
    mixed = residual.astype(jnp.float32) + projected
    totals = lax.psum(jnp.sum(mixed * mixed, axis=1), "head")
    inverse = lax.rsqrt(totals / (n_head * residual.shape[1]) + norm_epsilon)
    return (mixed * inverse[:, None] * gain.astype(jnp.float32)[None, :]).astype(jnp.bfloat16)


def solution(mesh):
    n_seq, n_head = mesh.shape["seq"], mesh.shape["head"]
    rows, wide = P(("rep", "seq"), "head"), P("head", None)
    in_specs = (rows, rows, rows, rows, wide, P("head"), P("rep"))
    if n_seq == 4 and n_head == 4:
        body = functools.partial(paired_body, n_seq, n_head, n_head // 2)
    else:
        body = functools.partial(gathered_body, n_head)
    return jax.shard_map(body, mesh=mesh, in_specs=in_specs, out_specs=rows, check_vma=False)
```
